32 devices in a mesh: row: 4 (over z), col: 8 (over y, x, core).
Axes of the slice: x: 2, y: 2, z: 4, core: 2. Of those that a mesh axis runs over, the one named last changes fastest.
Arguments:
- initial: bfloat16 [8, 24576], P(None, ('row', 'col')), may hold values from -8 to 8
- matrix: bfloat16 [24576, 24576], P('row', 'col'), may hold values from -1 to 4, as said below
Outputs:
- vectors: float32 [8, 24576], P(None, ('row', 'col'))
- estimates: float32 [4, 8], replicated
The draws below stay inside these ranges and needn't reach their ends.
Inputs may be any that keep to these rules, and one draw needn't show every extreme that they name: matrix is symmetric: entry (i, j) equals entry (j, i).
All inputs are finite; a program needn't handle non-finite values.
Results may differ from the reference program's by a relative error of at most 0.008.
Values may be sent and summed in bfloat16 or wider, within the bound.
A program may use at most 64 MiB of HBM per device.

```python
import math
import jax
import jax.numpy as jnp
from jax import lax

N = 24576
K = 8
ITERS = 4


def draw_initial(key, part):
    shared = jnp.clip(jax.random.normal(jax.random.fold_in(key, 11), (N,), jnp.float32), -3.0, 3.0)
    signs = jnp.where(jax.random.bernoulli(jax.random.fold_in(key, 12), 0.5, (K,)), 1.0, -1.0)
    weights = jax.random.uniform(jax.random.fold_in(key, 13), (K,), jnp.float32, 0.6, 1.4) * signs
    own_part = jnp.clip(jax.random.normal(jax.random.fold_in(key, 14), (K, N), jnp.float32), -3.0, 3.0) * 0.3
    return (weights[:, None] * shared[None, :] + own_part).astype(jnp.bfloat16)


def draw_matrix(key, part):
    tile_len = 256
    tile_count = N // tile_len

    def one_row(row_tile):

        def one_tile(col_tile):
            lesser = jnp.minimum(row_tile, col_tile)
            greater = jnp.maximum(row_tile, col_tile)
            subkey = jax.random.fold_in(key, lesser * tile_count + greater)
            entries = jax.random.normal(subkey, (tile_len, tile_len), jnp.float32)
            flipped = entries.T
            tile_block = jnp.where(row_tile < col_tile, entries, jnp.where(row_tile > col_tile, flipped, (entries + flipped) * 0.70710678))
            tile_block = tile_block / math.sqrt(N)
            shifts = jax.random.uniform(jax.random.fold_in(key, tile_count * tile_count + row_tile), (tile_len,), jnp.float32, 1.0, 3.0)
            on_diagonal = (row_tile == col_tile).astype(jnp.float32)
            tile_block = tile_block + on_diagonal * jnp.diag(shifts)
            return tile_block
        row_tiles = jax.vmap(one_tile)(jnp.arange(tile_count))
        return jnp.transpose(row_tiles, (1, 0, 2)).reshape(tile_len, N).astype(jnp.bfloat16)
    return lax.map(one_row, jnp.arange(tile_count)).reshape(N, N)


def setup_inputs(seed: int = 0) -> dict:
    key_list = jax.random.split(jax.random.key(seed), 3)
    return {
        "initial": draw_initial(jax.random.fold_in(key_list[2], 71), 0),
        "matrix": draw_matrix(jax.random.fold_in(key_list[2], 71), 0),
    }


def reference(initial, matrix):
    block = initial
    diagonals = []
    updated = jnp.zeros((K, N), jnp.float32)
    for iteration in range(ITERS):
        product = jnp.dot(block.astype(jnp.float32), matrix.astype(jnp.float32), preferred_element_type=jnp.float32)
        gram_matrix = jnp.dot(product, product.T, precision=lax.Precision.HIGHEST)
        factor = jnp.linalg.cholesky(gram_matrix)
        diagonals.append(jnp.diagonal(factor))
        updated = jax.scipy.linalg.solve_triangular(factor, product, lower=True)
        block = updated.astype(jnp.bfloat16)
    return (updated, jnp.stack(diagonals))
```

```python
import functools

import jax
import jax.numpy as jnp
from jax import lax
from jax.experimental import pallas as pl
from jax.experimental.pallas import tpu as pltpu
from jax.sharding import PartitionSpec as P

ITERS = 4
MESH = pl.DeviceIdType.MESH
LANES = 128
LIMBS = 2


def exchange(n, reduce_rows, last, rows, cols, x_ref, out_ref, est_ref, parts, full, grams,
             send1, recv1, send2, recv2, send3, recv3):
    r = lax.axis_index("row")
    c = lax.axis_index("col")
    total = rows * cols
    flat = r * cols + c
    me = r if reduce_rows else c
    k_vec = x_ref.shape[0]
    chunk = x_ref.shape[1] // n

    def member(j):
        return (j, c) if reduce_rows else (r, j)

    def device(i):
        return (i // cols, lax.rem(i, cols))

    barrier = pltpu.get_barrier_semaphore()
    for k in range(1, total):
        pl.semaphore_signal(
            barrier, inc=1, device_id=device(lax.rem(flat + k, total)), device_id_type=MESH
        )
    pl.semaphore_wait(barrier, total - 1)

    scatter = []
    for k in range(1, n):
        to = lax.rem(me + k, n)
        copy = pltpu.make_async_remote_copy(
            src_ref=x_ref.at[:, pl.ds(pl.multiple_of(to * chunk, LANES), chunk)],
            dst_ref=parts.at[k - 1],
            send_sem=send1.at[k - 1],
            recv_sem=recv1.at[k - 1],
            device_id=member(to),
            device_id_type=MESH,
        )
        copy.start()
        scatter.append(copy)
    summed = x_ref[:, pl.ds(pl.multiple_of(me * chunk, LANES), chunk)]
    for k in range(1, n):
        scatter[k - 1].wait_recv()
        summed = summed + parts[k - 1]

    gather = []
    if not last:
        full[me] = summed
        for k in range(1, n):
            copy = pltpu.make_async_remote_copy(
                src_ref=full.at[me],
                dst_ref=full.at[me],
                send_sem=send2.at[k - 1],
                recv_sem=recv2.at[k - 1],
                device_id=member(lax.rem(me + k, n)),
                device_id_type=MESH,
            )
            gather.append(copy)

    lane = lax.broadcasted_iota(jnp.int32, (k_vec, LANES), 1)
    sub = lax.broadcasted_iota(jnp.int32, (k_vec, LANES), 0)
    gram = jnp.zeros((k_vec, LANES), jnp.float32)
    for k in range(k_vec):
        column = jnp.sum(summed * summed[k:k + 1, :], axis=1, keepdims=True)
        gram = jnp.where(lane == k, column, gram)
    grams[flat] = gram
    share = []
    for k in range(1, total):
        copy = pltpu.make_async_remote_copy(
            src_ref=grams.at[flat],
            dst_ref=grams.at[flat],
            send_sem=send3.at[k - 1],
            recv_sem=recv3.at[k - 1],
            device_id=device(lax.rem(flat + k, total)),
            device_id_type=MESH,
        )
        copy.start()
        share.append(copy)
    for copy in gather:
        copy.start()
    for copy in share:
        copy.wait_recv()
    gram = grams[0]
    for k in range(1, total):
        gram = gram + grams[k]

    work = jnp.where(lane - k_vec == sub, 1.0, gram)
    est = jnp.zeros((k_vec, LANES), jnp.float32)
    scale = jnp.zeros((k_vec, LANES), jnp.float32)
    for k in range(k_vec):
        row = work[k:k + 1, :]
        pivot = row[:, k:k + 1]
        root = jnp.sqrt(pivot)
        est = jnp.where(lane == k, root, est)
        scale = jnp.where(sub == k, 1.0 / root, scale)
        factor = jnp.where(sub > k, work[:, k:k + 1] / pivot, 0.0)
        work = work - factor * row
    est_ref[...] = est
    inverse = work * scale
    columns = [inverse[:, k_vec + k:k_vec + k + 1] for k in range(k_vec)]

    def apply(block):
        result = columns[0] * block[0:1, :]
        for k in range(1, k_vec):
            result = result + columns[k] * block[k:k + 1, :]
        return result

    if last:
        out_ref[...] = apply(summed)
    else:
        for copy in gather:
            copy.wait_recv()
        for j in range(n):
            out_ref[:, j * chunk:(j + 1) * chunk] = apply(full[j]).astype(out_ref.dtype)
    for copy in scatter + gather + share:
        copy.wait_send()


def normalise(partial_sum, reduce_rows, last, collective_id):
    rows, cols = lax.axis_size("row"), lax.axis_size("col")
    n = rows if reduce_rows else cols
    k_vec, width = partial_sum.shape
    held = width // n
    chunk = pl.cdiv(held, LANES) * LANES
    padded = chunk != held
    if padded:
        partial_sum = jnp.pad(
            partial_sum.reshape(k_vec, n, held), ((0, 0), (0, 0), (0, chunk - held))
        ).reshape(k_vec, n * chunk)
    total = rows * cols
    if last:
        out = jax.ShapeDtypeStruct((k_vec, chunk), jnp.float32)
    else:
        out = jax.ShapeDtypeStruct((k_vec, n * chunk), jnp.bfloat16)
    dma = pltpu.SemaphoreType.DMA
    updated, est = pl.pallas_call(
        functools.partial(exchange, n, reduce_rows, last, rows, cols),
        out_shape=(out, jax.ShapeDtypeStruct((k_vec, LANES), jnp.float32)),
        in_specs=[pl.BlockSpec(memory_space=pltpu.VMEM)],
        out_specs=(pl.BlockSpec(memory_space=pltpu.VMEM),) * 2,
        scratch_shapes=[
            pltpu.VMEM((n - 1, k_vec, chunk), jnp.float32),
            pltpu.VMEM((n, k_vec, chunk), jnp.float32),
            pltpu.VMEM((total, k_vec, LANES), jnp.float32),
            dma((n - 1,)), dma((n - 1,)),
            dma((n - 1,)), dma((n - 1,)),
            dma((total - 1,)), dma((total - 1,)),
        ],
        compiler_params=pltpu.CompilerParams(
            collective_id=collective_id, has_side_effects=True
        ),
    )(partial_sum)
    if padded:
        updated = updated.reshape(k_vec, -1, chunk)[:, :, :held].reshape(k_vec, -1)
    return updated, est


def shards(initial, matrix):
    diagonals = []
    current = lax.all_gather(initial, "col", axis=1, tiled=True)
    for iteration in range(ITERS):
        reduce_rows = iteration % 2 == 0
        last = iteration == ITERS - 1
        contract = ((1,), (0,)) if reduce_rows else ((1,), (1,))
        partial_sum = lax.dot_general(
            current, matrix, (contract, ((), ())), preferred_element_type=jnp.float32
        )
        current, est = normalise(
            partial_sum, reduce_rows, last, 2 if last else (0 if reduce_rows else 1)
        )
        diagonals.append(est[0, :initial.shape[0]])
    return (current, jnp.stack(diagonals))


def update(work, k_vec, lane, sub):
    work = jnp.where(lane - k_vec == sub, 1.0, work)
    est = jnp.zeros((k_vec, LANES), jnp.float32)
    scale = jnp.zeros((k_vec, LANES), jnp.float32)
    for k in range(k_vec):
        row = work[k:k + 1, :]
        pivot = row[:, k:k + 1]
        root = jnp.sqrt(pivot)
        est = jnp.where(lane == k, root, est)
        scale = jnp.where(sub == k, 1.0 / root, scale)
        factor = jnp.where(sub > k, work[:, k:k + 1] / pivot, 0.0)
        work = work - factor * row
    inverse = work * scale
    return est, [inverse[:, k_vec + k:k_vec + k + 1] for k in range(k_vec)]


def fused(rows, cols, steps, first_ref, matrix_ref, out_ref, est_ref,
          mat, start, opened, block, early, ship, landed, full, grams, mine,
          load_sem, s0, r0, s1, r1, s2, r2, s3, r3):
    r = lax.axis_index("row")
    c = lax.axis_index("col")
    total = rows * cols
    flat = r * cols + c
    k_vec, held = first_ref.shape
    height, width = mat.shape
    piece = height // steps

    def device(i):
        return (i // cols, lax.rem(i, cols))

    def span(j, size):
        return pl.ds(pl.multiple_of(j * size, LANES), size)

    def load(i, p):
        window = (pl.ds(p * piece, piece), span(lax.rem(r + i, rows), held))
        return pltpu.make_async_copy(
            matrix_ref.at[window], mat.at[window], load_sem.at[(i - 1) * steps + p]
        )

    for i in range(1, rows + 1):
        for p in range(steps):
            load(i, p).start()

    barrier = pltpu.get_barrier_semaphore()

    def greet(k, carry):
        pl.semaphore_signal(
            barrier, inc=1, device_id=device(lax.rem(flat + k, total)), device_id_type=MESH
        )
        return carry

    lax.fori_loop(1, total, greet, 0)
    pl.semaphore_wait(barrier, total - 1)

    def opening(k):
        return pltpu.make_async_remote_copy(
            src_ref=first_ref, dst_ref=start.at[c], send_sem=s0.at[k - 1], recv_sem=r0.at[k - 1],
            device_id=(r, lax.rem(c + k, cols)), device_id_type=MESH,
        )

    for k in range(1, cols):
        opening(k).start()
    start[c] = first_ref[...]
    for k in range(1, cols):
        opening(k).wait_recv()
    for j in range(cols):
        opened[:, j * held:(j + 1) * held] = start[j]

    lane = lax.broadcasted_iota(jnp.int32, (k_vec, LANES), 1)
    sub = lax.broadcasted_iota(jnp.int32, (k_vec, LANES), 0)

    def split(slot, rest):
        for limb in range(LIMBS):
            part = rest.astype(block.dtype)
            block[slot, limb * k_vec:(limb + 1) * k_vec, :] = part
            rest = rest - part.astype(jnp.float32)

    unsent = []
    previous = None

    def fold(value):
        result = value[:k_vec]
        for limb in range(1, LIMBS):
            result = result + value[limb * k_vec:(limb + 1) * k_vec]
        return result

    def share(t, k):
        return pltpu.make_async_remote_copy(
            src_ref=mine.at[t], dst_ref=grams.at[t, k - 1], send_sem=s3.at[t], recv_sem=r3.at[t],
            device_id=device(lax.rem(flat + k, total)), device_id_type=MESH,
        )

    def arrival(t):
        everyone = grams.at[t, pl.ds(0, total - 1)]
        return pltpu.make_async_remote_copy(
            src_ref=everyone, dst_ref=everyone, send_sem=s3.at[t], recv_sem=r3.at[t],
            device_id=device(flat), device_id_type=MESH,
        )

    def inverse(t):
        arrival(t).wait_recv()
        spread = jnp.broadcast_to(mine[t] + jnp.sum(grams[t], axis=0), (k_vec, LANES))
        gram = jnp.zeros((k_vec, LANES), jnp.float32)
        for k in range(k_vec):
            column = jnp.sum(jnp.where(lane == k_vec * sub + k, spread, 0.0), axis=1, keepdims=True)
            gram = jnp.where(lane == k, column, gram)
        est, columns = update(gram, k_vec, lane, sub)
        est_ref[t:t + 1, :] = est[0:1, :k_vec]
        return columns

    def apply(columns, value):
        result = columns[0] * value[0:1, :]
        for k in range(1, k_vec):
            result = result + columns[k] * value[k:k + 1, :]
        return result

    for t in range(ITERS):
        down = t % 2 == 0
        last = t == ITERS - 1
        n = rows if down else cols
        me = r if down else c

        def member(j, down=down):
            return (j, c) if down else (r, j)

        def scatter(i, t=t, n=n, me=me, member=member):
            return pltpu.make_async_remote_copy(
                src_ref=ship.at[t, i - 1], dst_ref=landed.at[t, i - 1],
                send_sem=s1.at[t, i - 1], recv_sem=r1.at[t, i - 1],
                device_id=member(lax.rem(me + i, n)), device_id_type=MESH,
            )

        def gather(i, t=t, n=n, me=me, member=member):
            return pltpu.make_async_remote_copy(
                src_ref=full.at[t, me], dst_ref=full.at[t, me],
                send_sem=s2.at[t, i - 1], recv_sem=r2.at[t, i - 1],
                device_id=member(lax.rem(me + i, n)), device_id_type=MESH,
            )

        def terms(i, slots, t=t, down=down, n=n, me=me):
            j = lax.rem(me + i, n)
            m, mine_at = (cols, c) if down else (rows, r)
            acc = None
            for slot in slots:
                k = lax.rem(mine_at + slot, m)
                if down:
                    term = jnp.dot(block[slot], mat[span(k, held), span(j, held)],
                                   preferred_element_type=jnp.float32)
                else:
                    term = lax.dot_general(
                        block[slot], mat[span(j, held), span(k, held)], (((1,), (1,)), ((), ())),
                        preferred_element_type=jnp.float32)
                acc = term if acc is None else acc + term
            return fold(acc)

        def product(i, t=t, down=down, n=n, me=me, terms=terms):
            if t > 0:
                return early[i - 1] + terms(i, range(1, cols if down else rows))
            j = lax.rem(me + i, n)
            for p in range(steps):
                window = pl.ds(p * piece, piece)
                pltpu.make_async_copy(
                    matrix_ref.at[window, pl.ds(0, held)], mat.at[window, pl.ds(0, held)],
                    load_sem.at[(i - 1) * steps + p],
                ).wait()
            return jnp.dot(opened[...], mat[:, span(j, held)],
                           preferred_element_type=jnp.float32)

        if t > 0:
            def ahead(i, carry, terms=terms):
                early[i - 1] = terms(i, range(1))
                return carry

            lax.fori_loop(1, n + 1, ahead, 0, unroll=4)
            for i in range(1, previous[0]):
                previous[2](i).wait_recv()
            for slot in range(1, previous[0]):
                split(slot, full[t - 1, lax.rem(previous[1] + slot, previous[0])])

        def step(i, carry, t=t, product=product, scatter=scatter):
            ship[t, i - 1] = product(i)
            scatter(i).start()
            return carry

        lax.fori_loop(1, n, step, 0)
        summed = product(n)
        if t > 0:
            columns = inverse(t - 1)
        for i in range(1, n):
            scatter(i).wait_recv()
            summed = summed + landed[t, i - 1]
        if t > 0:
            summed = apply(columns, summed)

        if not last:
            full[t, me] = summed
            for i in range(1, n):
                gather(i).start()
        row = jnp.zeros((k_vec, LANES), jnp.float32)
        for k in range(k_vec):
            column = jnp.sum(summed * summed[k:k + 1, :], axis=1, keepdims=True)
            row = jnp.where(lane == k_vec * sub + k, column, row)
        mine[t] = jnp.sum(row, axis=0, keepdims=True)

        def shares(k, carry, t=t):
            share(t, k).start()
            return carry

        lax.fori_loop(1, total, shares, 0)
        if last:
            out_ref[...] = apply(inverse(t), summed)
        else:
            split(0, summed)
            previous = (n, me, gather)
        unsent += [scatter(i) for i in range(1, n)]
        if not last:
            unsent += [gather(i) for i in range(1, n)]
    for copy in unsent:
        copy.wait_send()
    for t in range(ITERS):
        arrival(t).wait_send()
    for k in range(1, cols):
        opening(k).wait_send()


def whole(initial, matrix):
    rows, cols = lax.axis_size("row"), lax.axis_size("col")
    k_vec, held = initial.shape
    height, width = matrix.shape
    total = rows * cols
    most = max(rows, cols)
    steps = 4
    dma = pltpu.SemaphoreType.DMA
    return pl.pallas_call(
        functools.partial(fused, rows, cols, steps),
        out_shape=(jax.ShapeDtypeStruct((k_vec, held), jnp.float32),
                   jax.ShapeDtypeStruct((ITERS, k_vec), jnp.float32)),
        in_specs=[pl.BlockSpec(memory_space=pltpu.VMEM), pl.BlockSpec(memory_space=pl.ANY)],
        out_specs=(pl.BlockSpec(memory_space=pltpu.VMEM),) * 2,
        scratch_shapes=[
            pltpu.VMEM((height, width), matrix.dtype),
            pltpu.VMEM((cols, k_vec, held), initial.dtype),
            pltpu.VMEM((k_vec, height), initial.dtype),
            pltpu.VMEM((most, LIMBS * k_vec, held), initial.dtype),
            pltpu.VMEM((most, k_vec, held), jnp.float32),
            pltpu.VMEM((ITERS, most - 1, k_vec, held), jnp.float32),
            pltpu.VMEM((ITERS, most - 1, k_vec, held), jnp.float32),
            pltpu.VMEM((ITERS, most, k_vec, held), jnp.float32),
            pltpu.VMEM((ITERS, total - 1, 1, LANES), jnp.float32),
            pltpu.VMEM((ITERS, 1, LANES), jnp.float32),
            dma((rows * steps,)),
            dma((cols - 1,)), dma((cols - 1,)),
            dma((ITERS, most - 1)), dma((ITERS, most - 1)),
            dma((ITERS, most - 1)), dma((ITERS, most - 1)),
            dma((ITERS,)), dma((ITERS,)),
        ],
        compiler_params=pltpu.CompilerParams(
            collective_id=0, has_side_effects=True, vmem_limit_bytes=60 * 2**20
        ),
    )(initial, matrix)


def program(initial, matrix):
    k_vec, held = initial.shape
    resident = matrix.size * matrix.dtype.itemsize <= 40 * 2**20
    if held % LANES == 0 and k_vec * k_vec <= LANES and resident:
        return whole(initial, matrix)
    return shards(initial, matrix)


def solution(mesh):
    return jax.shard_map(
        program,
        mesh=mesh,
        in_specs=(P(None, ("row", "col")), P("row", "col")),
        out_specs=(P(None, ("row", "col")), P()),
        check_vma=False,
    )
```
